32 devices in a mesh: rep: 8 (over y, x, core), ep: 4 (over z).
Axes of the slice: x: 2, y: 2, z: 4, core: 2. Of those that a mesh axis runs over, the one named last changes fastest.
Arguments:
- tokens: bfloat16 [2, 512, 4096], P(None, 'ep', 'rep'), may hold values from -6 to 6
- expert_ids: int32 [2, 512, 2], P(None, 'ep'), may hold values from 0 to 3, all different within a row; in each aligned block of 128 rows (0 to 127, 128 to 255, ..., all dimensions but the last counted through in order) at most 96 rows name the same one
- router_weight: bfloat16 [4096, 4], P('rep'), may hold values from -0.09375 to 0.09375
- w_gate: bfloat16 [4, 4096, 8192], P('ep', None, 'rep'), may hold values from -0.09375 to 0.09375
- w_up: bfloat16 [4, 4096, 8192], P('ep', None, 'rep'), may hold values from -0.09375 to 0.09375
- w_down: bfloat16 [4, 8192, 4096], P('ep', 'rep'), may hold values from -0.0625 to 0.0625
- cotangent: bfloat16 [2, 512, 4096], P(None, 'ep', 'rep'), may hold values from -6 to 6
Outputs:
- mixed: bfloat16 [2, 512, 4096], P(None, 'ep', 'rep')
- token_grad: bfloat16 [2, 512, 4096], P(None, 'ep', 'rep')
- gate_grad: bfloat16 [4, 4096, 8192], P('ep', None, 'rep')
- up_grad: bfloat16 [4, 4096, 8192], P('ep', None, 'rep')
- down_grad: bfloat16 [4, 8192, 4096], P('ep', 'rep')
- router_grad: float32 [4096, 4], P('rep')
The draws below stay inside these ranges and needn't reach their ends.
Inputs may be any that keep to these rules, and one draw needn't show every extreme that they name: `expert_ids`: each row names 2 different experts. Among the 128 rows of one index of ep in one microbatch no expert is named by more than 96 rows, and in every draw some expert is named by exactly 96 of them.
All inputs are finite; a program needn't handle non-finite values.
Results may differ from the reference program's by a relative error of at most 0.025.
Values may be sent and summed in bfloat16 or wider, within the bound.
A program may use at most 192 MiB of HBM per device.

```python
import math
import jax
import jax.numpy as jnp
import numpy as np
from jax import lax

D = 4096
FF = 8192
EXPERTS = 4
TOP = 2
TOK_DEV = 128
MICRO = 2
CAP = 96
TOKENS = 512
N_REP = 8
N_EP = 4


def shard_levels(own_key, shape, shards, low, largest):
    factor_of, own = 1.0, jax.random.fold_in(own_key, 6)
    for axis_at, blocks in shards:
        draws = jnp.exp(jax.random.uniform(jax.random.fold_in(own, axis_at), (blocks,), jnp.float32, low / len(shards), largest / len(shards)))
        factor_of = factor_of * jnp.repeat(draws, shape[axis_at] // blocks).reshape([-1 if axis == axis_at else 1 for axis in range(len(shape))])
    return factor_of


def shared_out(rng, own, number, rows, number_of, top, reach, skew):
    sequence = jax.random.permutation(rng, number_of)
    packed, ordinary = shares(number_of, rows * top, reach, skew, True), shares(number_of, rows * top, reach, skew, False)
    places = jnp.arange(number_of)

    def named(tallies, turn):
        used = int((tallies > 0).sum())
        fixed = max(1, used // 4)
        passed = fixed + (places - fixed + turn * (used - fixed)) % max(1, number_of - fixed)
        return jnp.zeros((number_of,), jnp.int32).at[sequence[jnp.where(places < fixed, places, passed)]].set(jnp.asarray(tallies, jnp.int32))

    tallies = jnp.where(number % 4 == 0, named(packed, number // 4), named(ordinary, number - number // 4 - 1))
    mixed = jax.random.permutation(jax.random.fold_in(own, 3), number_of)
    donor, sink = mixed[0:number_of // 2 * 2:2], mixed[1:number_of // 2 * 2:2]
    room = jnp.minimum(tallies[donor] - 1, reach - tallies[sink]) // 2
    room = jnp.where((donor == sequence[0]) | (sink == sequence[0]) | (tallies[sink] == 0), 0, jnp.maximum(room, 0))
    passed = jax.random.randint(jax.random.fold_in(own, 4), (number_of // 2,), 0, 1 << 20) % (room + 1)
    tallies = tallies.at[donor].add(-passed).at[sink].add(passed)
    members = jnp.searchsorted(jnp.cumsum(tallies), jnp.arange(rows * top), side="right").astype(jnp.int32)
    listing = members.reshape(top, rows).T
    listing = listing[jax.random.permutation(jax.random.fold_in(own, 1), rows)]
    turn = jax.random.randint(jax.random.fold_in(own, 2), (rows, 1), 0, top)
    return jnp.take_along_axis(listing, (jnp.arange(top)[None, :] + turn) % top, axis=1)


def shares(number_of, total, reach, skew, full):
    weights = [(1 << 20) // math.isqrt(standing ** skew) + 1 for standing in range(1, number_of + 1)]
    largest = reach if full else min(reach, max(-(-total // number_of), total * weights[0] // sum(weights)))
    least = 1 if total - largest >= number_of - 1 else 0
    holding, rest = [largest] + [least] * (number_of - 1), total - largest - least * (number_of - 1)
    while rest > 0:
        candidates = [i for i in range(1, number_of) if holding[i] < largest] or [i for i in range(1, number_of) if holding[i] < reach]
        whole, budget = sum([weights[i] for i in candidates]), rest
        for i in candidates:
            addition = min(reach - holding[i], max(1, budget * weights[i] // whole), rest)
            holding[i] = holding[i] + addition
            rest = rest - addition
    return np.array(holding)


def normal_values(rng, dims, scale, bound, shards=(), kind=jnp.bfloat16):
    entries = jax.random.normal(rng, dims, jnp.float32) * scale
    if len(shards) > 0:
        entries = shard_levels(rng, dims, shards, -0.22, 0.18) * entries
    return jnp.clip(entries, min=-bound, max=bound).astype(kind)


def setup_inputs(seed: int = 0) -> dict:
    splits = jax.random.split(jax.random.key(seed), 8)
    tokens = normal_values(splits[0], (MICRO, TOKENS, D), 1.0, 6.0, ((1, 4), (2, 8)))
    expert_ids_keys = jax.random.split(jax.random.fold_in(splits[1], 1), MICRO * TOKENS // TOK_DEV)
    expert_ids_turns = jax.random.permutation(jax.random.fold_in(splits[1], 3), MICRO * TOKENS // TOK_DEV)
    expert_ids = jax.vmap(lambda own, number: shared_out(jax.random.fold_in(splits[1], 2), own, number, TOK_DEV, EXPERTS, TOP, CAP, 2))(expert_ids_keys, expert_ids_turns).reshape((MICRO, TOKENS, TOP))
    router_weight = normal_values(splits[2], (D, EXPERTS), D ** -0.5, 0.09375, ((0, 8),))
    w_gate = normal_values(splits[3], (EXPERTS, D, FF), D ** -0.5, 0.09375, ((0, 4), (2, 8)))
    w_up = normal_values(splits[4], (EXPERTS, D, FF), D ** -0.5, 0.09375, ((0, 4), (2, 8)))
    w_down = normal_values(splits[5], (EXPERTS, FF, D), FF ** -0.5, 0.0625, ((0, 4), (1, 8)))
    cotangent = normal_values(splits[6], (MICRO, TOKENS, D), 1.0, 6.0, ((1, 4), (2, 8)))
    return dict(tokens=tokens, expert_ids=expert_ids, router_weight=router_weight, w_gate=w_gate, w_up=w_up, w_down=w_down, cotangent=cotangent)


def positions(route_ids):
    hits = route_ids[:, :, None] == jnp.arange(EXPERTS, dtype=jnp.int32)[None, None, :]
    per_token = jnp.sum(hits.astype(jnp.int32), axis=1)
    before = jnp.cumsum(per_token, axis=0) - per_token
    return jnp.sum(jnp.where(hits, before[:, None, :], 0), axis=2).astype(jnp.int32)


def widen(value):
    return lax.optimization_barrier(value.astype(jnp.bfloat16)).astype(jnp.float32)


def expert_forward(rows_in, gate_w, up_w):
    pre_gate = jnp.dot(rows_in, gate_w, preferred_element_type=jnp.float32)
    pre_up = jnp.dot(rows_in, up_w, preferred_element_type=jnp.float32)
    hidden = (jax.nn.silu(pre_gate) * pre_up).astype(jnp.bfloat16)
    return pre_gate, pre_up, hidden


def grouped_down(hidden, down_w):
    group = FF // N_REP
    slots = hidden.shape[0]
    parts_h = hidden.reshape(slots, N_REP, group).transpose(1, 0, 2)
    parts_w = down_w.reshape(N_REP, group, D)

    def add(total, pair):
        return total + widen(jnp.dot(pair[0], pair[1], preferred_element_type=jnp.float32)), None

    total, _ = lax.scan(add, jnp.zeros((slots, D), jnp.float32), (parts_h, parts_w))
    return total.astype(jnp.bfloat16)


def grouped_in(gate_part, up_part, gate_w, up_w):
    group = FF // N_REP
    slots = gate_part.shape[0]
    parts_g = gate_part.reshape(slots, N_REP, group).transpose(1, 0, 2)
    parts_u = up_part.reshape(slots, N_REP, group).transpose(1, 0, 2)
    weights_g = gate_w.reshape(D, N_REP, group).transpose(1, 0, 2)
    weights_u = up_w.reshape(D, N_REP, group).transpose(1, 0, 2)

    def add(total, items):
        term = jnp.dot(items[0], items[2].T, preferred_element_type=jnp.float32)
        term = term + jnp.dot(items[1], items[3].T, preferred_element_type=jnp.float32)
        return total + widen(term), None

    total, _ = lax.scan(add, jnp.zeros((slots, D), jnp.float32), (parts_g, parts_u, weights_g, weights_u))
    return total.astype(jnp.bfloat16)


def reference(tokens, expert_ids, router_weight, w_gate, w_up, w_down, cotangent):
    slot_count = N_EP * CAP
    source = jnp.arange(TOKENS, dtype=jnp.int32) // TOK_DEV
    plans = []
    inputs = []
    for step in range(MICRO):
        route_ids = expert_ids[step].astype(jnp.int32)
        places = jax.vmap(positions)(route_ids.reshape(N_EP, TOK_DEV, TOP)).reshape(TOKENS, TOP)
        row_ids = (source[:, None] * CAP + places).astype(jnp.int32)
        values = jnp.broadcast_to(tokens[step][:, None, :], (TOKENS, TOP, D))
        inputs.append(jnp.zeros((EXPERTS, slot_count, D), jnp.bfloat16).at[route_ids, row_ids].set(values))
        plans.append((route_ids, row_ids))
    expert_in = jnp.stack(inputs, axis=1)

    def forward_one(items):
        rows_all, gate_w, up_w, down_w = items
        outs = []
        for step in range(MICRO):
            pre_gate, pre_up, hidden = expert_forward(rows_all[step], gate_w, up_w)
            outs.append(grouped_down(hidden, down_w))
        return jnp.stack(outs)

    expert_out = lax.map(forward_one, (expert_in, w_gate, w_up, w_down))
    mixed = []
    cots = []
    logit_grads = []
    router_grad = jnp.zeros((D, EXPERTS), jnp.float32)
    for step in range(MICRO):
        route_ids, row_ids = plans[step]
        logits = jnp.dot(tokens[step], router_weight, preferred_element_type=jnp.float32)
        hits = route_ids[:, :, None] == jnp.arange(EXPERTS, dtype=jnp.int32)[None, None, :]
        chosen = jnp.sum(jnp.where(hits, logits[:, None, :], 0.0), axis=2)
        spread = chosen[:, 0] - chosen[:, 1]
        gates = jnp.stack([jax.nn.sigmoid(spread), jax.nn.sigmoid(-spread)], axis=1)
        pairs = expert_out[:, step][route_ids, row_ids].astype(jnp.float32)
        mixed.append((gates[:, 0, None] * pairs[:, 0] + gates[:, 1, None] * pairs[:, 1]).astype(jnp.bfloat16))
        cot = cotangent[step].astype(jnp.float32)
        gate_dots = jnp.sum(cot[:, None, :] * pairs, axis=2)
        delta = (gate_dots[:, 0] - gate_dots[:, 1]) * gates[:, 0] * gates[:, 1]
        logit_grad = delta[:, None] * (hits[:, 0].astype(jnp.float32) - hits[:, 1].astype(jnp.float32))
        logit_grads.append(logit_grad)
        router_grad = router_grad + jnp.dot(tokens[step].astype(jnp.float32).T, logit_grad, precision=lax.Precision.HIGHEST)
        cot_pairs = (gates[:, :, None] * cot[:, None, :]).astype(jnp.bfloat16)
        cots.append(jnp.zeros((EXPERTS, slot_count, D), jnp.bfloat16).at[route_ids, row_ids].set(cot_pairs))
    expert_cot = jnp.stack(cots, axis=1)

    def backward_one(items):
        rows_all, cots_all, gate_w, up_w, down_w = items
        gate_acc = jnp.zeros((D, FF), jnp.float32)
        up_acc = jnp.zeros((D, FF), jnp.float32)
        down_acc = jnp.zeros((FF, D), jnp.float32)
        grads_in = []
        for step in range(MICRO):
            rows_in = rows_all[step]
            cot_rows = cots_all[step]
            pre_gate, pre_up, hidden = expert_forward(rows_in, gate_w, up_w)
            hidden_grad = jnp.dot(cot_rows, down_w.T, preferred_element_type=jnp.float32)
            gate_sig = jax.nn.sigmoid(pre_gate)
            gate_act = pre_gate * gate_sig
            pre_gate_grad = (hidden_grad * pre_up * (gate_sig * (1.0 + pre_gate * (1.0 - gate_sig)))).astype(jnp.bfloat16)
            pre_up_grad = (hidden_grad * gate_act).astype(jnp.bfloat16)
            down_acc = down_acc + jnp.dot(hidden.T, cot_rows, preferred_element_type=jnp.float32)
            gate_acc = gate_acc + jnp.dot(rows_in.T, pre_gate_grad, preferred_element_type=jnp.float32)
            up_acc = up_acc + jnp.dot(rows_in.T, pre_up_grad, preferred_element_type=jnp.float32)
            grads_in.append(grouped_in(pre_gate_grad, pre_up_grad, gate_w, up_w))
        return gate_acc.astype(jnp.bfloat16), up_acc.astype(jnp.bfloat16), down_acc.astype(jnp.bfloat16), jnp.stack(grads_in)

    gate_grad, up_grad, down_grad, expert_in_grad = lax.map(backward_one, (expert_in, expert_cot, w_gate, w_up, w_down))
    token_grad = []
    for step in range(MICRO):
        route_ids, row_ids = plans[step]
        pairs = expert_in_grad[:, step][route_ids, row_ids].astype(jnp.float32)
        router_in = jnp.dot(logit_grads[step], router_weight.astype(jnp.float32).T, precision=lax.Precision.HIGHEST)
        token_grad.append((pairs[:, 0] + pairs[:, 1] + router_in).astype(jnp.bfloat16))
    return jnp.stack(mixed), jnp.stack(token_grad), gate_grad, up_grad, down_grad, router_grad
```

```python
import jax
import jax.numpy as jnp
from jax import lax
from jax.sharding import Mesh, PartitionSpec as P

TOP = 2
CORES = 2
F32 = jnp.float32
BF16 = jnp.bfloat16


def contract(left, right, left_dim, right_dim):
    return lax.dot_general(
        left, right, (((left_dim,), (right_dim,)), ((), ())), preferred_element_type=F32
    )


def swap(value, cores):
    return lax.ppermute(value, "core", [(i, cores - 1 - i) for i in range(cores)])


def gather_features(rows, core, earlier=None):
    mine = lax.all_gather(rows, "chip", axis=0, tiled=False)
    if earlier is not None:
        mine = after(mine, earlier)
    other = swap(mine, CORES)
    pieces = []
    for chip in range(mine.shape[0]):
        pieces.append(jnp.where(core == 0, mine[chip], other[chip]))
        pieces.append(jnp.where(core == 0, other[chip], mine[chip]))
    return jnp.concatenate(pieces, axis=1)


def core_parts(partial, core):
    chips = lax.axis_size("chip")
    width = partial.shape[1] // (chips * CORES)
    pieces = [
        lax.slice_in_dim(partial, i * width, (i + 1) * width, axis=1) for i in range(chips * CORES)
    ]
    low, high = jnp.stack(pieces[0::2]), jnp.stack(pieces[1::2])
    return jnp.where(core == 0, low, high), jnp.where(core == 0, high, low)


def pair_sum(keep, send):
    return (keep.astype(F32) + swap(send, CORES).astype(F32)).astype(BF16)


def scatter_chips(total):
    return lax.psum_scatter(total, "chip", scatter_dimension=0, tiled=False)


def exchange(rows, sign):
    count = lax.axis_size("ep")
    blocks = rows.reshape(count, -1, rows.shape[-1])
    moved = [blocks[0]]
    for d in range(1, count):
        pairs = [(i, (i + sign * d) % count) for i in range(count)]
        moved.append(lax.ppermute(blocks[d], "ep", pairs))
    return jnp.concatenate(moved, axis=0)


def after(value, earlier):
    zero = earlier[(0,) * earlier.ndim].astype(F32) * 0.0
    return value + zero.astype(value.dtype)


def route(ids, experts, capacity):
    micro, rows, _ = ids.shape
    away = lax.rem(ids - lax.axis_index("ep") + experts, experts)
    hits = ids[..., None] == jnp.arange(experts, dtype=jnp.int32)
    per_token = jnp.sum(hits.astype(F32), axis=2)
    earlier = (
        jnp.arange(rows)[:, None] > jnp.arange(rows)[None, :]
    ).astype(BF16)
    before = jnp.einsum(
        "ij,mje->mie", earlier, per_token.astype(BF16), preferred_element_type=F32
    )
    places = jnp.sum(jnp.where(hits, before[:, :, None, :], 0.0), axis=3).astype(jnp.int32)
    step = jnp.arange(micro, dtype=jnp.int32)[:, None, None]
    slots = ((away * micro + step) * capacity + places).reshape(micro * rows, TOP)
    picks = slots[:, :, None] == jnp.arange(experts * micro * capacity, dtype=jnp.int32)
    return hits.reshape(micro * rows, TOP, experts), picks[:, 0], picks[:, 1]


def shards(tokens, expert_ids, router_weight, w_gate, w_up, w_down, cotangent):
    micro, rows, width = tokens.shape
    experts = router_weight.shape[1]
    capacity = min(rows, 3 * rows * TOP // (2 * experts))
    core = lax.axis_index("core")
    gate_w, up_w, down_w = w_gate[0], w_up[0], w_down[0]
    toks = tokens.reshape(micro * rows, width)
    cots = cotangent.reshape(micro * rows, width)

    hits, pick0, pick1 = route(expert_ids, experts, capacity)
    hot0, hot1 = pick0.astype(BF16), pick1.astype(BF16)
    hot = hot0 + hot1

    moved_rows = exchange(contract(hot, toks, 0, 0).astype(BF16), 1)

    partial_logits = contract(router_weight, toks, 0, 1)
    logits = lax.psum(after(partial_logits, moved_rows), ("chip", "core")).T
    chosen = jnp.sum(jnp.where(hits, logits[:, None, :], 0.0), axis=2)
    spread = chosen[:, 0] - chosen[:, 1]
    first = jax.nn.sigmoid(spread)
    second = jax.nn.sigmoid(-spread)
    slot_gate = jnp.sum(
        jnp.where(pick0, first[:, None], 0.0) + jnp.where(pick1, second[:, None], 0.0), axis=0
    )
    sent_cots = (contract(hot, cots, 0, 0) * slot_gate[:, None]).astype(BF16)
    moved_cots = exchange(sent_cots, 1)

    expert_rows = gather_features(moved_rows, core, moved_cots)
    pre_gate = contract(expert_rows, gate_w, 1, 0)
    pre_up = contract(expert_rows, up_w, 1, 0)
    gate_sig = jax.nn.sigmoid(pre_gate)
    gate_act = pre_gate * gate_sig
    hidden = (gate_act * pre_up).astype(BF16)
    keep, send = core_parts(contract(hidden, down_w, 1, 0).astype(BF16), core)
    total = pair_sum(keep, send)
    expert_cots = after(gather_features(moved_cots, core, hidden), total)
    returned = exchange(after(scatter_chips(total), slot_gate), -1)

    hidden_grad = contract(expert_cots, down_w, 1, 1)
    gate_pre_grad = (
        hidden_grad * pre_up * (gate_sig * (1.0 + pre_gate * (1.0 - gate_sig)))
    ).astype(BF16)
    up_pre_grad = (hidden_grad * gate_act).astype(BF16)
    inputs = (contract(gate_pre_grad, gate_w, 1, 1) + contract(up_pre_grad, up_w, 1, 1)).astype(BF16)
    keep_in, send_in = core_parts(inputs, core)
    scattered_in = scatter_chips(pair_sum(keep_in, send_in))

    down_grad = contract(hidden, expert_cots, 0, 0).astype(BF16)
    gate_grad = contract(expert_rows, gate_pre_grad, 0, 0).astype(BF16)
    up_grad = contract(expert_rows, up_pre_grad, 0, 0).astype(BF16)

    first_out = contract(hot0, returned, 1, 0)
    second_out = contract(hot1, returned, 1, 0)
    mixed = (first[:, None] * first_out + second[:, None] * second_out).astype(BF16)
    cot_wide = cots.astype(F32)
    partial_dots = jnp.sum(cot_wide * (first_out - second_out), axis=1)
    partial_dots = after(partial_dots, slot_gate)
    gate_dots = lax.psum(partial_dots, ("chip", "core"))
    delta = gate_dots * first * second
    logit_grad = delta[:, None] * (hits[:, 0].astype(F32) - hits[:, 1].astype(F32))
    router_grad = lax.psum(
        lax.dot_general(
            logit_grad, toks.astype(F32), (((0,), (0,)), ((), ())), precision=lax.Precision.HIGHEST
        ),
        "ep",
    ).T
    router_in = lax.dot_general(
        logit_grad,
        router_weight.astype(F32),
        (((1,), (1,)), ((), ())),
        precision=lax.Precision.HIGHEST,
    )
    returned_grad = exchange(after(scattered_in, router_grad), -1)
    token_grad = (contract(hot, returned_grad, 1, 0) + router_in).astype(BF16)
    return (
        mixed.reshape(tokens.shape),
        token_grad.reshape(tokens.shape),
        gate_grad[None],
        up_grad[None],
        down_grad[None],
        router_grad,
    )


def solution(mesh):
    rep, ep = mesh.shape["rep"], mesh.shape["ep"]
    inner = Mesh(mesh.devices.reshape(rep // CORES, CORES, ep), ("chip", "core", "ep"))
    reps = ("chip", "core")
    in_specs = (
        P(None, "ep", reps),
        P(None, "ep", None),
        P(reps, None),
        P("ep", None, reps),
        P("ep", None, reps),
        P("ep", reps, None),
        P(None, "ep", reps),
    )
    out_specs = (
        P(None, "ep", reps),
        P(None, "ep", reps),
        P("ep", None, reps),
        P("ep", None, reps),
        P("ep", reps, None),
        P(reps, None),
    )
    return jax.shard_map(shards, mesh=inner, in_specs=in_specs, out_specs=out_specs, check_vma=False)
```
